256 devices in a mesh: blk: 32 (over y_lo, z, core), tp: 8 (over x, y_hi).
Axes of the slice: x: 4, y: 4 (y_hi: 2, y_lo: 2; y = y_hi * 2 + y_lo), z: 8, core: 2. Of those that a mesh axis runs over, the one named last changes fastest.
Arguments:
- dec_states: bfloat16 [8192, 5120], P('blk', 'tp'), may hold values from -200 to 200
- norm_gain: float32 [5120], replicated, may hold values from 0.1 to 1.9
- query_weight: bfloat16 [5120, 3072], P(None, 'tp'), may hold values from -0.078125 to 0.078125
- out_weight: bfloat16 [3072, 5120], P('tp'), may hold values from -0.109375 to 0.109375
- enc_keys: bfloat16 [12288, 3072], P('blk', 'tp'), may hold values from -1000 to 1000
- enc_values: bfloat16 [12288, 3072], P('blk', 'tp'), may hold values from -6 to 6
Outputs:
- attn_out: bfloat16 [8192, 5120], P('blk', 'tp')
The draws below stay inside these ranges and needn't reach their ends.
All inputs are finite; a program needn't handle non-finite values.
Results may differ from the reference program's by a relative error of at most 0.034.
Values may be sent and summed in bfloat16 or wider, within the bound.
A program may use at most 128 MiB of HBM per device.

```python
import math
import jax
import jax.numpy as jnp
from jax import lax

D = 5120
HEAD_DIM = 128
Q_DEV = 256
HEADS = 24
DEC_TOK = 8192
ENC_TOK = 12288


def draw_dec_states(key, part):
    key_base, key_rows, key_cols = jax.random.split(key, 3)
    base = jnp.clip(jax.random.normal(key_base, (DEC_TOK, D), jnp.float32), -6.0, 6.0)
    row_scale = jnp.exp(jax.random.uniform(key_rows, (DEC_TOK, 1), jnp.float32) * jnp.log(10.0))
    ramp = 1.0 + 2.0 * jnp.arange(D, dtype=jnp.float32) / D
    col_scale = jnp.exp(jax.random.uniform(key_cols, (1, D), jnp.float32) * jnp.log(10.0)) * ramp[None, :]
    return (base * row_scale * col_scale / 10.0).astype(jnp.bfloat16)


def draw_enc_keys(key, part):
    key_base = jax.random.fold_in(key, 0)
    base = jnp.clip(jax.random.normal(key_base, (ENC_TOK, HEADS * HEAD_DIM), jnp.float32), -6.0, 6.0)
    return base.astype(jnp.bfloat16)


def shard_levels(key, shape, cuts, low, top_value):
    gain = 1.0
    for dim, parts in cuts:
        draws = jax.random.uniform(jax.random.fold_in(jax.random.fold_in(key, 6), dim), (parts,), jnp.float32, low / len(cuts), top_value / len(cuts))
        gain = gain * jnp.repeat(jnp.exp(draws), shape[dim] // parts).reshape((-1,) + (1,) * (len(shape) - 1 - dim))
    return gain


def noise(rng, extent, width, most, pieces=(), kind=jnp.bfloat16):
    values = jax.random.normal(rng, extent, jnp.float32) * width
    if len(pieces) > 0:
        values = shard_levels(rng, extent, pieces, -0.22, 0.18) * values
    return jnp.clip(values, min=-most, max=most).astype(kind)


def setup_inputs(seed: int = 0) -> dict:
    arg_keys = jax.random.split(jax.random.key(seed), 7)
    dec_states = draw_dec_states(jax.random.fold_in(arg_keys[6], 71), 0)
    norm_gain = jnp.clip(1.0 + 0.18 * jax.random.normal(arg_keys[1], (D,), jnp.float32), 0.1, 1.9)
    query_weight = noise(arg_keys[2], (D, HEADS * HEAD_DIM), D ** -0.5, 0.078125, ((1, 8),))
    out_weight = noise(arg_keys[3], (HEADS * HEAD_DIM, D), (HEADS * HEAD_DIM) ** -0.5, 0.109375, ((0, 8),))
    enc_keys = draw_enc_keys(jax.random.fold_in(arg_keys[6], 71), 0)
    enc_values = noise(arg_keys[5], (ENC_TOK, HEADS * HEAD_DIM), 1.0, 6.0, ((0, 32), (1, 8)))
    return {"dec_states": dec_states, "norm_gain": norm_gain, "query_weight": query_weight, "out_weight": out_weight, "enc_keys": enc_keys, "enc_values": enc_values}


NORM_EPS = 1e-06

def reference(dec_states, norm_gain, query_weight, out_weight, enc_keys, enc_values):
    states = dec_states.astype(jnp.float32)
    mean_sq = lax.optimization_barrier(jnp.mean(states * states, axis=1, keepdims=True))
    normed = (states * lax.rsqrt(mean_sq + NORM_EPS) * norm_gain.astype(jnp.float32)).astype(jnp.bfloat16)
    queries = jnp.dot(normed, query_weight, preferred_element_type=jnp.float32).astype(jnp.bfloat16)
    query_heads = queries.reshape(DEC_TOK // Q_DEV, Q_DEV, HEADS, HEAD_DIM).transpose(2, 0, 1, 3)
    key_heads = enc_keys.reshape(ENC_TOK, HEADS, HEAD_DIM).transpose(1, 0, 2)
    value_heads = enc_values.reshape(ENC_TOK, HEADS, HEAD_DIM).transpose(1, 0, 2)
    score_scale = 1.0 / math.sqrt(HEAD_DIM)

    def one_head(operands):
        query_blocks, key_rows, value_rows = operands

        def one_block(query_rows):
            scores = jnp.dot(query_rows, key_rows.T, preferred_element_type=jnp.float32) * score_scale
            row_peak = lax.optimization_barrier(jnp.max(scores, axis=1, keepdims=True))
            exp_scores = jnp.exp(scores - row_peak)
            row_total = lax.optimization_barrier(jnp.sum(exp_scores, axis=1, keepdims=True))
            mixed = jnp.dot(exp_scores.astype(jnp.bfloat16), value_rows, preferred_element_type=jnp.float32)
            return mixed / row_total
        return lax.map(one_block, query_blocks)
    attended = lax.map(one_head, (query_heads, key_heads, value_heads))
    attended = attended.transpose(1, 2, 0, 3).reshape(DEC_TOK, HEADS * HEAD_DIM).astype(jnp.bfloat16)
    return jnp.dot(attended, out_weight, preferred_element_type=jnp.float32).astype(jnp.bfloat16)
```

```python
import math

import jax
import jax.numpy as jnp
from jax import lax
from jax.experimental import pallas as pl
from jax.experimental.pallas import tpu as pltpu
from jax.sharding import PartitionSpec as P

HD = 128
NORM_EPS = 1e-06
MESH = pl.DeviceIdType.MESH
NZ, NX = 8, 4
F32, BF16 = jnp.float32, jnp.bfloat16
LOG2E = 1.4426950408889634


def body(x_hbm, gain_ref, wq_hbm, wo_hbm, k_hbm, v_hbm, out_ref,
         kbuf, vbuf, vtmp, xbuf, wq, wobuf, qacc, ssacc, qbuf, acc, mbuf, lbuf,
         osend, ssend, orecv, srecv, att, oacc,
         lsem, zss, zrs, bss, brs, xss, xrs, wss, wrs, wbs, wbr, qss, qrs,
         oss, ors, ass, ars):
    rows, xcols = x_hbm.shape
    toks = k_hbm.shape[0]
    heads = k_hbm.shape[1] // HD
    half = rows // 2
    blk, tp = lax.axis_index("blk"), lax.axis_index("tp")
    c = lax.rem(blk, 2)
    z = lax.rem(blk // 2, NZ)
    yl = blk // (2 * NZ)
    x, yh = tp // 2, lax.rem(tp, 2)

    def zdev(d):
        return ((yl * NZ + lax.rem(z + d + NZ, NZ)) * 2 + c, tp)

    def tpdev(dx, dy):
        return (blk, lax.rem(x + dx + NX, NX) * 2 + lax.rem(yh + dy, 2))

    def tpi(dx, dy):
        return lax.rem(x + dx + NX, NX) * 2 + lax.rem(yh + dy, 2)

    sib = (blk + 1 - 2 * c, tp)
    ypart = (blk + 2 * NZ - 4 * NZ * yl, tp)
    zsrc = lambda d: lax.rem(z + d + NZ, NZ)
    others = [(dx, dy) for dy in (0, 1) for dx in (0, 1, 3, 2) if (dx, dy) != (0, 0)]
    sends = []

    def rcopy(src, dst, ss, rs, dev):
        return pltpu.make_async_remote_copy(
            src_ref=src, dst_ref=dst, send_sem=ss, recv_sem=rs,
            device_id=dev, device_id_type=MESH)

    def send(src, dst, ss, rs, dev):
        cp = rcopy(src, dst, ss, rs, dev)
        cp.start()
        sends.append(cp)

    def await_recv(dst, ss, rs):
        rcopy(dst, dst, ss, rs, sib).wait_recv()

    def kslot(h, zz, cc):
        return kbuf.at[h, zz, pl.ds(cc * toks, toks), :]

    def vslot(h, zz, cc):
        return vbuf.at[h, zz, cc]

    kl = [pltpu.make_async_copy(k_hbm.at[:, pl.ds(h * HD, HD)], kslot(h, z, c), lsem.at[h]) for h in range(heads)]
    vl = [pltpu.make_async_copy(v_hbm.at[:, pl.ds(h * HD, HD)], vtmp.at[h], lsem.at[3 + h]) for h in range(heads)]
    xl = pltpu.make_async_copy(x_hbm, xbuf.at[tp], lsem.at[6])
    wql = pltpu.make_async_copy(wq_hbm, wq, lsem.at[7])
    wol = pltpu.make_async_copy(wo_hbm.at[:, :, pl.ds(pl.multiple_of(tp * xcols, HD), xcols)], wobuf.at[:, tp], lsem.at[8])
    kl[0].start()
    vl[0].start()
    xl.start()
    for h in range(1, heads):
        kl[h].start()
        vl[h].start()
    wql.start()
    wol.start()

    bar = pltpu.get_barrier_semaphore()
    peers = [zdev(1), zdev(-1), sib, ypart] + [tpdev(dx, dy) for dx, dy in others]
    for dev in peers:
        pl.semaphore_signal(bar, inc=1, device_id=dev, device_id_type=MESH)
    pl.semaphore_wait(bar, len(peers))

    def zsend(h, s, d, kv):
        src_z = zsrc(-s if d == 0 else s)
        ref = kslot(h, src_z, c) if kv == 0 else vslot(h, src_z, c)
        send(ref, ref, zss.at[d, s, h, kv], zrs.at[d, s, h, kv], zdev(1 if d == 0 else -1))

    def bsend(h, src_z, slot, kv):
        ref = kslot(h, src_z, c) if kv == 0 else vslot(h, src_z, c)
        send(ref, ref, bss.at[slot, h, kv], brs.at[slot, h, kv], sib)

    def own(h):
        kl[h].wait()
        zsend(h, 0, 0, 0)
        vl[h].wait()
        vbuf[h, z, c] = vtmp[h].T
        zsend(h, 0, 1, 1)
        zsend(h, 0, 0, 1)
        zsend(h, 0, 1, 0)
        bsend(h, z, 0, 0)
        bsend(h, z, 0, 1)

    def slot_of(d, s):
        return 2 * s - 1 + d if s < 4 else 7

    def arrive(h, s):
        order = [(0, 0), (1, 1), (0, 1), (1, 0)]
        for d, kv in order:
            if s == 4 and kv != d:
                continue
            src_z = zsrc(-s if d == 0 else s)
            ref = kslot(h, src_z, c) if kv == 0 else vslot(h, src_z, c)
            await_recv(ref, zss.at[d, s - 1, h, kv], zrs.at[d, s - 1, h, kv])
            if s < 3 or (s == 3 and kv == d):
                zsend(h, s, d, kv)
            bsend(h, src_z, slot_of(d, s), kv)

    def sib_arrive(h, s):
        if s == 0:
            lst = [(z, 0)]
        elif s == 4:
            lst = [(zsrc(4), 7)]
        else:
            lst = [(zsrc(-s), slot_of(0, s)), (zsrc(s), slot_of(1, s))]
        for src_z, slot in lst:
            await_recv(kslot(h, src_z, 1 - c), bss.at[slot, h, 0], brs.at[slot, h, 0])
            await_recv(vslot(h, src_z, 1 - c), bss.at[slot, h, 1], brs.at[slot, h, 1])

    XOWN_R, XOWN_L, XY, XP_R, XP_L, XOH_R, XOH_L, XPH_R, XPH_L = range(9)

    def xsend(ref, i, dx, dy):
        send(ref, ref, xss.at[i], xrs.at[i], tpdev(dx, dy))

    def xwait(ref, i):
        await_recv(ref, xss.at[i], xrs.at[i])

    def xfull(t):
        return xbuf.at[t]

    def xtop(t):
        return xbuf.at[t, pl.ds(0, half), :]

    def xbot(t):
        return xbuf.at[t, pl.ds(half, half), :]

    def qblock(t, first=False):
        xf = xbuf[t].astype(F32)
        sq = xf * xf
        part = sq[:, 0:HD]
        for j in range(1, xcols // HD):
            part = part + sq[:, j * HD:(j + 1) * HD]
        g = gain_ref[:, pl.ds(pl.multiple_of(t * xcols, HD), xcols)]
        xg = (xf * g).astype(BF16)
        prod = jnp.dot(xg, wq[t], preferred_element_type=F32)
        if first:
            ssacc[...] = part
            qacc[...] = prod
        else:
            ssacc[...] += part
            qacc[...] += prod

    def init_state():
        mbuf[...] = jnp.full(mbuf.shape, -1e30, F32)
        lbuf[...] = jnp.zeros(lbuf.shape, F32)
        acc[...] = jnp.zeros(acc.shape, F32)

    def tile(h, zz, r):
        s = lax.dot_general(kbuf[h, zz], qbuf[h, r], (((1,), (1,)), ((), ())), preferred_element_type=F32)
        mo = mbuf[h, r]
        mn = jnp.maximum(mo, jnp.max(s, axis=0, keepdims=True))
        p = jnp.exp2(s - mn)
        f = jnp.exp2(mo - mn)
        lbuf[h, r] = lbuf[h, r] * f + jnp.sum(p, axis=0, keepdims=True)
        vv = jnp.concatenate([vbuf[h, zz, 0], vbuf[h, zz, 1]], axis=1)
        o = jnp.dot(vv, p.astype(BF16), preferred_element_type=F32)
        acc[h, r] = acc[h, r] * f + o
        mbuf[h, r] = mn

    def tiles(h, z0, n, stride, r0, nr):
        def step(i, carry):
            tile(h, zsrc(z0 + stride * (i // nr)), r0 + lax.rem(i, nr))
            return carry
        lax.fori_loop(0, n * nr, step, 0)

    def finish_partner(h):
        osend[h] = acc[h, 1].astype(BF16)
        ssend[h, 0:1] = mbuf[h, 1]
        ssend[h, 1:2] = lbuf[h, 1]
        send(osend.at[h], orecv.at[h], oss.at[h, 0], ors.at[h, 0], ypart)
        send(ssend.at[h], srecv.at[h], oss.at[h, 1], ors.at[h, 1], ypart)

    def merge(h):
        await_recv(orecv.at[h], oss.at[h, 0], ors.at[h, 0])
        await_recv(srecv.at[h], oss.at[h, 1], ors.at[h, 1])
        ma, mb = mbuf[h, 0], srecv[h, 0:1]
        m = jnp.maximum(ma, mb)
        fa, fb = jnp.exp2(ma - m), jnp.exp2(mb - m)
        tot = lbuf[h, 0] * fa + srecv[h, 1:2] * fb
        o = (acc[h, 0] * fa + orecv[h].astype(F32) * fb) / tot
        att[h, tp] = o.T.astype(BF16)
        for i, (dx, dy) in enumerate(others):
            send(att.at[h, tp], att.at[h, tp], ass.at[h, i], ars.at[h, i], tpdev(dx, dy))

    def out_part(h, first=False):
        for i, (dx, dy) in enumerate(others):
            t = tpi(-dx, dy)
            await_recv(att.at[h, t], ass.at[h, i], ars.at[h, i])
        a = jnp.concatenate([att[h, t] for t in range(8)], axis=1)
        w = wobuf[h].reshape(8 * HD, xcols)
        prod = jnp.dot(a, w, preferred_element_type=F32)
        if first:
            oacc[...] = prod
        else:
            oacc[...] += prod

    hh = HD // 2

    def wslot(t, cc):
        return wobuf.at[:, t, pl.ds(cc * hh, hh), :]

    def wsend():
        for i, (dx, dy) in enumerate(others):
            t = tpi(dx, dy)
            src = wo_hbm.at[:, pl.ds(c * hh, hh), pl.ds(pl.multiple_of(t * xcols, HD), xcols)]
            send(src, wslot(tp, c), wss.at[i], wrs.at[i], tpdev(dx, dy))

    def wfwd():
        for i, (dx, dy) in enumerate(others):
            t = tpi(-dx, dy)
            await_recv(wslot(t, c), wss.at[i], wrs.at[i])
            send(wslot(t, c), wslot(t, c), wbs.at[i], wbr.at[i], sib)

    def wdone():
        wol.wait()
        for i, (dx, dy) in enumerate(others):
            t = tpi(-dx, dy)
            await_recv(wslot(t, 1 - c), wbs.at[i], wbr.at[i])

    tl, tr, t2 = tpi(-1, 0), tpi(1, 0), tpi(2, 0)
    pt, ptl, ptr, pt2 = tpi(0, 1), tpi(-1, 1), tpi(1, 1), tpi(2, 1)

    own(0)
    xl.wait()
    xsend(xfull(tp), XOWN_R, 1, 0)
    xsend(xfull(tp), XOWN_L, -1, 0)
    xsend(xfull(tp), XY, 0, 1)
    own(1)
    init_state()
    wql.wait()
    qblock(tp, True)
    arrive(0, 1)
    own(2)
    xwait(xfull(tl), XOWN_R)
    xsend(xtop(tl), XOH_R, 1, 0)
    xwait(xfull(tr), XOWN_L)
    xsend(xbot(tr), XOH_L, -1, 0)
    xwait(xfull(pt), XY)
    xsend(xfull(pt), XP_R, 1, 0)
    xsend(xfull(pt), XP_L, -1, 0)
    qblock(tl)
    qblock(tr)
    qblock(pt)
    arrive(0, 2)
    xwait(xtop(t2), XOH_R)
    xwait(xbot(t2), XOH_L)
    qblock(t2)
    arrive(1, 1)
    xwait(xfull(ptl), XP_R)
    xsend(xtop(ptl), XPH_R, 1, 0)
    xwait(xfull(ptr), XP_L)
    xsend(xbot(ptr), XPH_L, -1, 0)
    wsend()
    qblock(ptl)
    qblock(ptr)
    arrive(0, 3)
    arrive(1, 2)
    xwait(xtop(pt2), XPH_R)
    xwait(xbot(pt2), XPH_L)
    qblock(pt2)

    mean_sq = jnp.sum(ssacc[...], axis=1, keepdims=True) * (1.0 / (8 * xcols))
    scale = lax.rsqrt(mean_sq + NORM_EPS) * (LOG2E / math.sqrt(HD))
    for h in range(heads):
        qbuf[h, 0] = (qacc[:, h * HD:(h + 1) * HD] * scale).astype(BF16)
        send(qbuf.at[h, 0], qbuf.at[h, 1], qss.at[h], qrs.at[h], ypart)

    def qwait(h):
        await_recv(qbuf.at[h, 1], qss.at[h], qrs.at[h])

    arrive(0, 4)
    for s in range(5):
        sib_arrive(0, s)
    tiles(0, 0, 8, 1, 0, 1)
    arrive(2, 1)
    for s in range(2):
        sib_arrive(1, s)
        sib_arrive(2, s)
    tiles(1, -1, 3, 1, 0, 1)
    qwait(0)
    tiles(0, 0, 8, 1, 1, 1)
    finish_partner(0)
    arrive(1, 3)
    tiles(2, -1, 3, 1, 0, 1)
    qwait(1)
    tiles(1, -1, 3, 1, 1, 1)
    merge(0)
    arrive(2, 2)
    sib_arrive(1, 2)
    tiles(1, -2, 2, 4, 0, 2)
    qwait(2)
    tiles(2, -1, 3, 1, 1, 1)
    arrive(1, 4)
    sib_arrive(1, 3)
    sib_arrive(1, 4)
    tiles(1, 3, 3, 1, 0, 2)
    arrive(2, 3)
    finish_partner(1)
    sib_arrive(2, 2)
    tiles(2, -2, 2, 4, 0, 2)
    merge(1)
    arrive(2, 4)
    sib_arrive(2, 3)
    tiles(2, -3, 2, 6, 0, 2)
    sib_arrive(2, 4)
    tiles(2, 4, 1, 1, 0, 2)
    finish_partner(2)
    wfwd()
    merge(2)
    wdone()
    out_part(0, True)
    out_part(1)
    out_part(2)
    out_ref[...] = oacc[...].astype(BF16)
    for cp in sends:
        cp.wait_send()


def per_device(dec_states, norm_gain, query_weight, out_weight, enc_keys, enc_values):
    rows, xcols = dec_states.shape
    toks, width = enc_keys.shape
    heads = width // HD
    vm = pltpu.VMEM
    dma = pltpu.SemaphoreType.DMA
    hbm = pl.BlockSpec(memory_space=pl.ANY)
    inv = pl.BlockSpec(memory_space=pltpu.VMEM)
    return pl.pallas_call(
        body,
        out_shape=jax.ShapeDtypeStruct((rows, xcols), BF16),
        in_specs=[hbm, inv, hbm, hbm, hbm, hbm],
        out_specs=inv,
        scratch_shapes=[
            vm((heads, NZ, 2 * toks, HD), BF16),
            vm((heads, NZ, 2, HD, toks), BF16),
            vm((heads, toks, HD), BF16),
            vm((8, rows, xcols), BF16),
            vm((8, xcols, width), BF16),
            vm((heads, 8, HD, xcols), BF16),
            vm((rows, width), F32),
            vm((rows, HD), F32),
            vm((heads, 2, rows, HD), BF16),
            vm((heads, 2, HD, rows), F32),
            vm((heads, 2, 1, rows), F32),
            vm((heads, 2, 1, rows), F32),
            vm((heads, HD, rows), BF16),
            vm((heads, 8, rows), F32),
            vm((heads, HD, rows), BF16),
            vm((heads, 8, rows), F32),
            vm((heads, 8, rows, HD), BF16),
            vm((rows, xcols), F32),
            dma((9,)),
            dma((2, 4, heads, 2)), dma((2, 4, heads, 2)),
            dma((8, heads, 2)), dma((8, heads, 2)),
            dma((9,)), dma((9,)),
            dma((7,)), dma((7,)),
            dma((7,)), dma((7,)),
            dma((heads,)), dma((heads,)),
            dma((heads, 2)), dma((heads, 2)),
            dma((heads, 7)), dma((heads, 7)),
        ],
        compiler_params=pltpu.CompilerParams(
            collective_id=0, has_side_effects=True, vmem_limit_bytes=60 * 2**20),
    )(
        dec_states,
        norm_gain.reshape(1, -1),
        query_weight.reshape(8, xcols, width),
        out_weight.reshape(heads, HD, 8 * xcols),
        enc_keys,
        enc_values,
    )


def solution(mesh):
    in_specs = (P("blk", "tp"), P(), P(None, "tp"), P("tp", None), P("blk", "tp"), P("blk", "tp"))
    return jax.shard_map(
        per_device, mesh=mesh, in_specs=in_specs, out_specs=P("blk", "tp"), check_vma=False
    )
```

```python
import math

import jax
import jax.numpy as jnp
from jax import lax
from jax.experimental import pallas as pl
from jax.experimental.pallas import tpu as pltpu
from jax.sharding import PartitionSpec as P

HD = 128
NORM_EPS = 1e-06
MESH = pl.DeviceIdType.MESH
NZ, NX = 8, 4
F32, BF16 = jnp.float32, jnp.bfloat16
LOG2E = 1.4426950408889634


def body(x_hbm, gain_ref, wq_hbm, wo_hbm, k_hbm, v_hbm, out_ref,
         kbuf, vbuf, vtmp, xbuf, wq, wobuf, qacc, ssacc, qbuf, acc, mbuf, lbuf,
         osend, ssend, orecv, srecv, att, oacc, wst,
         sbuf, lsem, zss, zrs, bss, brs, xss, xrs, wss, wrs, wbs, wbr, wys, wyr, qss, qrs,
         oss, ors, ass, ars):
    rows, xcols = x_hbm.shape
    toks = k_hbm.shape[0]
    heads = k_hbm.shape[1] // HD
    half = rows // 2
    blk, tp = lax.axis_index("blk"), lax.axis_index("tp")
    c = lax.rem(blk, 2)
    z = lax.rem(blk // 2, NZ)
    yl = blk // (2 * NZ)
    x, yh = tp // 2, lax.rem(tp, 2)

    def zdev(d):
        return ((yl * NZ + lax.rem(z + d + NZ, NZ)) * 2 + c, tp)

    def tpdev(dx, dy):
        return (blk, lax.rem(x + dx + NX, NX) * 2 + lax.rem(yh + dy, 2))

    def tpi(dx, dy):
        return lax.rem(x + dx + NX, NX) * 2 + lax.rem(yh + dy, 2)

    sib = (blk + 1 - 2 * c, tp)
    ypart = (blk + 2 * NZ - 4 * NZ * yl, tp)
    zsrc = lambda d: lax.rem(z + d + NZ, NZ)
    DX = (1, 3, 2)
    sends = []

    def rcopy(src, dst, ss, rs, dev):
        return pltpu.make_async_remote_copy(
            src_ref=src, dst_ref=dst, send_sem=ss, recv_sem=rs,
            device_id=dev, device_id_type=MESH)

    def send(src, dst, ss, rs, dev):
        cp = rcopy(src, dst, ss, rs, dev)
        cp.start()
        sends.append(cp)

    def await_recv(dst, ss, rs):
        rcopy(dst, dst, ss, rs, sib).wait_recv()

    def kslot(h, zz, cc):
        return kbuf.at[h, zz, pl.ds(cc * toks, toks), :]

    def vslot(h, zz, cc):
        return vbuf.at[h, zz, cc]

    kl = [pltpu.make_async_copy(k_hbm.at[:, pl.ds(h * HD, HD)], kslot(h, z, c), lsem.at[h]) for h in range(heads)]
    vl = [pltpu.make_async_copy(v_hbm.at[:, pl.ds(h * HD, HD)], vtmp.at[h], lsem.at[3 + h]) for h in range(heads)]
    xl = pltpu.make_async_copy(x_hbm, xbuf.at[tp], lsem.at[6])
    wql = pltpu.make_async_copy(wq_hbm, wq, lsem.at[7])
    wol = pltpu.make_async_copy(wo_hbm.at[:, :, pl.ds(pl.multiple_of(tp * xcols, HD), xcols)], wobuf.at[:, tp], lsem.at[8])
    kl[0].start()
    vl[0].start()
    xl.start()
    for h in range(1, heads):
        kl[h].start()
        vl[h].start()
    wql.start()
    wol.start()

    bar = pltpu.get_barrier_semaphore()
    peers = [zdev(1), zdev(-1), sib, ypart, tpdev(0, 1)] + [tpdev(dx, 0) for dx in DX]
    for dev in peers:
        pl.semaphore_signal(bar, inc=1, device_id=dev, device_id_type=MESH)
    pl.semaphore_wait(bar, len(peers))

    def zsend(h, s, d, kv):
        src_z = zsrc(-s if d == 0 else s)
        ref = kslot(h, src_z, c) if kv == 0 else vslot(h, src_z, c)
        send(ref, ref, zss.at[d, s, h, kv], zrs.at[d, s, h, kv], zdev(1 if d == 0 else -1))

    def bsend(h, src_z, slot, kv):
        ref = kslot(h, src_z, c) if kv == 0 else vslot(h, src_z, c)
        send(ref, ref, bss.at[slot, h, kv], brs.at[slot, h, kv], sib)

    def own(h):
        kl[h].wait()
        zsend(h, 0, 0, 0)
        vl[h].wait()
        vbuf[h, z, c] = vtmp[h].T
        zsend(h, 0, 1, 1)
        zsend(h, 0, 0, 1)
        zsend(h, 0, 1, 0)
        bsend(h, z, 0, 0)
        bsend(h, z, 0, 1)

    def slot_of(d, s):
        return 2 * s - 1 + d if s < 4 else 7

    def arrive(h, s):
        order = [(0, 0), (1, 1), (0, 1), (1, 0)]
        for d, kv in order:
            if s == 4 and kv != d:
                continue
            src_z = zsrc(-s if d == 0 else s)
            ref = kslot(h, src_z, c) if kv == 0 else vslot(h, src_z, c)
            await_recv(ref, zss.at[d, s - 1, h, kv], zrs.at[d, s - 1, h, kv])
            if s < 3 or (s == 3 and kv == d):
                zsend(h, s, d, kv)
            bsend(h, src_z, slot_of(d, s), kv)

    def sib_arrive(h, s):
        if s == 0:
            lst = [(z, 0)]
        elif s == 4:
            lst = [(zsrc(4), 7)]
        else:
            lst = [(zsrc(-s), slot_of(0, s)), (zsrc(s), slot_of(1, s))]
        for src_z, slot in lst:
            await_recv(kslot(h, src_z, 1 - c), bss.at[slot, h, 0], brs.at[slot, h, 0])
            await_recv(vslot(h, src_z, 1 - c), bss.at[slot, h, 1], brs.at[slot, h, 1])

    XOWN_R, XOWN_L, XY, XP_R, XP_L, XOH_R, XOH_L, XPH_R, XPH_L = range(9)

    def xsend(ref, i, dx, dy):
        send(ref, ref, xss.at[i], xrs.at[i], tpdev(dx, dy))

    def xwait(ref, i):
        await_recv(ref, xss.at[i], xrs.at[i])

    def xfull(t):
        return xbuf.at[t]

    def xtop(t):
        return xbuf.at[t, pl.ds(0, half), :]

    def xbot(t):
        return xbuf.at[t, pl.ds(half, half), :]

    def qblock(t, first=False):
        xf = xbuf[t].astype(F32)
        sq = xf * xf
        part = sq[:, 0:HD]
        for j in range(1, xcols // HD):
            part = part + sq[:, j * HD:(j + 1) * HD]
        g = gain_ref[:, pl.ds(pl.multiple_of(t * xcols, HD), xcols)]
        xg = (xf * g).astype(BF16)
        prod = jnp.dot(xg, wq[t], preferred_element_type=F32)
        if first:
            ssacc[...] = part
            qacc[...] = prod
        else:
            ssacc[...] += part
            qacc[...] += prod

    def init_state():
        mbuf[...] = jnp.full(mbuf.shape, -1e30, F32)
        lbuf[...] = jnp.zeros(lbuf.shape, F32)
        acc[...] = jnp.zeros(acc.shape, F32)

    def update(h, r, s, vv):
        mo = mbuf[h, r]
        mn = jnp.maximum(mo, jnp.max(s, axis=0, keepdims=True))
        p = jnp.exp2(s - mn).astype(BF16)
        f = jnp.exp2(mo - mn)
        ones = jnp.ones((16, vv.shape[1]), BF16)
        o = jnp.dot(jnp.concatenate([vv, ones], axis=0), p, preferred_element_type=F32)
        lbuf[h, r] = lbuf[h, r] * f + o[HD:HD + 1]
        acc[h, r] = acc[h, r] * f + o[:HD]
        mbuf[h, r] = mn

    cur = []

    def feed(h, d):
        zz = zsrc(d)
        par = (cur[0][2] + 1) % 2 if cur else 0
        old = cur.pop() if cur else None
        vv = None if old is None else values(old[0], old[1])
        for r in range(2):
            sbuf[2 * par + r] = scores(h, zz, r)
            if old is not None:
                update(old[0], r, sbuf[2 * old[2] + r], vv)
        cur.append((h, zz, par))

    def flush():
        h, zz, par = cur.pop()
        vv = values(h, zz)
        for r in range(2):
            update(h, r, sbuf[2 * par + r], vv)

    def flush_last():
        h, zz, par = cur.pop()
        vv = values(h, zz)
        update(h, 1, sbuf[2 * par + 1], vv)
        finish_partner(h)
        update(h, 0, sbuf[2 * par], vv)

    def scores(h, zz, r):
        return lax.dot_general(kbuf[h, zz], qbuf[h, r], (((1,), (1,)), ((), ())), preferred_element_type=F32)

    def values(h, zz):
        return jnp.concatenate([vbuf[h, zz, 0], vbuf[h, zz, 1]], axis=1)

    def finish_partner(h):
        osend[h] = acc[h, 1].astype(BF16)
        ssend[h, 0:1] = mbuf[h, 1]
        ssend[h, 1:2] = lbuf[h, 1]
        send(osend.at[h], orecv.at[h], oss.at[h, 0], ors.at[h, 0], ypart)
        send(ssend.at[h], srecv.at[h], oss.at[h, 1], ors.at[h, 1], ypart)

    def merge(h):
        await_recv(orecv.at[h], oss.at[h, 0], ors.at[h, 0])
        await_recv(srecv.at[h], oss.at[h, 1], ors.at[h, 1])
        ma, mb = mbuf[h, 0], srecv[h, 0:1]
        m = jnp.maximum(ma, mb)
        fa, fb = jnp.exp2(ma - m), jnp.exp2(mb - m)
        tot = lbuf[h, 0] * fa + srecv[h, 1:2] * fb
        o = (acc[h, 0] * fa + orecv[h].astype(F32) * fb) / tot
        att[h, tp] = o.T.astype(BF16)
        att_send(h, tp, 0)
        att_one(h, tp, 3, 0, 1)

    def att_one(h, t, i, dx, dy):
        send(att.at[h, t], att.at[h, t], ass.at[h, i], ars.at[h, i], tpdev(dx, dy))

    def att_send(h, t, base):
        for i, dx in enumerate(DX):
            att_one(h, t, base + i, dx, 0)

    def att_wait(h, i, dx, dy):
        await_recv(att.at[h, tpi(-dx, dy)], ass.at[h, i], ars.at[h, i])

    def att_relay(h):
        att_wait(h, 3, 0, 1)
        att_send(h, tpi(0, 1), 4)

    def out_part(h, first=False):
        for i, dx in enumerate(DX):
            att_wait(h, i, dx, 0)
        for i, dx in enumerate(DX):
            att_wait(h, 4 + i, dx, 1)
        a = jnp.concatenate([att[h, t] for t in range(8)], axis=1)
        w = wobuf[h].reshape(8 * HD, xcols)
        prod = jnp.dot(a, w, preferred_element_type=F32)
        if first:
            oacc[...] = prod
        else:
            oacc[...] += prod

    hh = HD // 4

    def wslot(t, cc, yy):
        return wobuf.at[:, t, pl.ds((2 * cc + yy) * hh, hh), :]

    def wsrc(t):
        return wo_hbm.at[:, pl.ds((2 * c + yl) * hh, hh), pl.ds(pl.multiple_of(t * xcols, HD), xcols)]

    def w_own(i):
        send(wsrc(tpi(DX[i], 0)), wslot(tp, c, yl), wss.at[i], wrs.at[i], tpdev(DX[i], 0))

    def w_y():
        for i, dx in enumerate(DX):
            send(wsrc(tpi(dx, 1)), wst.at[i], wss.at[7 + i], wrs.at[7 + i], tpdev(0, 1))
        send(wsrc(tpi(0, 1)), wslot(tp, c, yl), wss.at[6], wrs.at[6], tpdev(0, 1))

    def w_relay(i):
        await_recv(wst.at[i], wss.at[7 + i], wrs.at[7 + i])
        send(wst.at[i], wslot(tpi(0, 1), c, yl), wss.at[3 + i], wrs.at[3 + i], tpdev(DX[i], 0))

    def w_from(i):
        return tpi(0, 1) if i == 6 else tpi(-DX[i % 3], i // 3)

    def wfwd(i):
        ref = wslot(w_from(i), c, yl)
        await_recv(ref, wss.at[i], wrs.at[i])
        send(ref, ref, wys.at[i], wyr.at[i], ypart)
        send(ref, ref, wbs.at[0, i], wbr.at[0, i], sib)

    def wfwd2():
        for i in W_ORDER:
            ref = wslot(w_from(i), c, 1 - yl)
            await_recv(ref, wys.at[i], wyr.at[i])
            send(ref, ref, wbs.at[1, i], wbr.at[1, i], sib)

    def wdone():
        wol.wait()
        for j in range(2):
            for i in W_ORDER:
                ref = wslot(w_from(i), 1 - c, yl if j == 0 else 1 - yl)
                await_recv(ref, wbs.at[j, i], wbr.at[j, i])

    W_ORDER = (0, 1, 6, 2, 3, 4, 5)
    tl, tr, t2 = tpi(-1, 0), tpi(1, 0), tpi(2, 0)
    pt, ptl, ptr, pt2 = tpi(0, 1), tpi(-1, 1), tpi(1, 1), tpi(2, 1)

    own(0)
    xl.wait()
    xsend(xfull(tp), XOWN_R, 1, 0)
    xsend(xfull(tp), XOWN_L, -1, 0)
    xsend(xfull(tp), XY, 0, 1)
    own(1)
    w_y()
    w_own(0)
    w_own(1)
    init_state()
    wql.wait()
    qblock(tp, True)
    arrive(0, 1)
    own(2)
    xwait(xfull(tl), XOWN_R)
    xsend(xtop(tl), XOH_R, 1, 0)
    xwait(xfull(tr), XOWN_L)
    xsend(xbot(tr), XOH_L, -1, 0)
    xwait(xfull(pt), XY)
    xsend(xfull(pt), XP_R, 1, 0)
    xsend(xfull(pt), XP_L, -1, 0)
    qblock(tl)
    qblock(tr)
    qblock(pt)
    arrive(0, 2)
    arrive(1, 1)
    xwait(xtop(t2), XOH_R)
    xwait(xbot(t2), XOH_L)
    qblock(t2)
    wfwd(0)
    wfwd(1)
    xwait(xfull(ptl), XP_R)
    xsend(xtop(ptl), XPH_R, 1, 0)
    xwait(xfull(ptr), XP_L)
    xsend(xbot(ptr), XPH_L, -1, 0)
    w_own(2)
    qblock(ptl)
    qblock(ptr)
    arrive(0, 3)
    w_relay(0)
    w_relay(1)
    w_relay(2)
    wfwd(6)
    arrive(1, 2)
    arrive(2, 1)
    xwait(xtop(pt2), XPH_R)
    xwait(xbot(pt2), XPH_L)
    qblock(pt2)

    mean_sq = jnp.sum(ssacc[...], axis=1, keepdims=True) * (1.0 / (8 * xcols))
    scale = lax.rsqrt(mean_sq + NORM_EPS) * (LOG2E / math.sqrt(HD))
    for h in range(heads):
        qbuf[h, 0] = (qacc[:, h * HD:(h + 1) * HD] * scale).astype(BF16)
        send(qbuf.at[h, 0], qbuf.at[h, 1], qss.at[h], qrs.at[h], ypart)

    def qwait(h):
        await_recv(qbuf.at[h, 1], qss.at[h], qrs.at[h])

    arrive(0, 4)
    for st in range(5):
        sib_arrive(0, st)
    qwait(0)
    feed(0, 0)
    feed(0, -1)
    feed(0, 1)
    arrive(1, 3)
    wfwd(3)
    feed(0, -2)
    feed(0, 2)
    feed(0, -3)
    wfwd(2)
    feed(0, 3)
    feed(0, 4)
    sib_arrive(1, 0)
    sib_arrive(1, 1)
    qwait(1)
    feed(1, 0)
    finish_partner(0)
    arrive(2, 2)
    feed(1, -1)
    feed(1, 1)
    sib_arrive(1, 2)
    feed(1, -2)
    feed(1, 2)
    arrive(1, 4)
    sib_arrive(1, 3)
    feed(1, -3)
    feed(1, 3)
    sib_arrive(1, 4)
    feed(1, 4)
    qwait(2)
    sib_arrive(2, 0)
    sib_arrive(2, 1)
    feed(2, 0)
    finish_partner(1)
    merge(0)
    arrive(2, 3)
    feed(2, -1)
    feed(2, 1)
    wfwd(4)
    sib_arrive(2, 2)
    feed(2, -2)
    feed(2, 2)
    sib_arrive(2, 3)
    feed(2, -3)
    feed(2, 3)
    merge(1)
    flush()
    att_relay(0)
    wfwd(5)
    arrive(2, 4)
    sib_arrive(2, 4)
    feed(2, 4)
    flush_last()
    att_relay(1)
    wfwd2()
    merge(2)
    att_relay(2)
    wdone()
    out_part(0, True)
    out_part(1)
    out_part(2)
    out_ref[...] = oacc[...].astype(BF16)
    for cp in sends:
        cp.wait_send()


def per_device(dec_states, norm_gain, query_weight, out_weight, enc_keys, enc_values):
    rows, xcols = dec_states.shape
    toks, width = enc_keys.shape
    heads = width // HD
    vm = pltpu.VMEM
    dma = pltpu.SemaphoreType.DMA
    hbm = pl.BlockSpec(memory_space=pltpu.HBM)
    inv = pl.BlockSpec(memory_space=pltpu.VMEM)
    return pl.pallas_call(
        body,
        out_shape=pltpu.VMEM((rows, xcols), BF16),
        in_specs=[hbm, inv, hbm, hbm, hbm, hbm],
        out_specs=inv,
        scratch_shapes=[
            vm((heads, NZ, 2 * toks, HD), BF16),
            vm((heads, NZ, 2, HD, toks), BF16),
            vm((heads, toks, HD), BF16),
            vm((8, rows, xcols), BF16),
            vm((8, xcols, width), BF16),
            vm((heads, 8, HD, xcols), BF16),
            vm((rows, width), F32),
            vm((rows, HD), F32),
            vm((heads, 2, rows, HD), BF16),
            vm((heads, 2, HD, rows), F32),
            vm((heads, 2, 1, rows), F32),
            vm((heads, 2, 1, rows), F32),
            vm((heads, HD, rows), BF16),
            vm((heads, 8, rows), F32),
            vm((heads, HD, rows), BF16),
            vm((heads, 8, rows), F32),
            vm((heads, 8, rows, HD), BF16),
            vm((rows, xcols), F32),
            vm((3, heads, HD // 4, xcols), BF16),
            vm((4, 2 * toks, rows), F32),
            dma((9,)),
            dma((2, 4, heads, 2)), dma((2, 4, heads, 2)),
            dma((8, heads, 2)), dma((8, heads, 2)),
            dma((9,)), dma((9,)),
            dma((10,)), dma((10,)),
            dma((2, 7)), dma((2, 7)),
            dma((7,)), dma((7,)),
            dma((heads,)), dma((heads,)),
            dma((heads, 2)), dma((heads, 2)),
            dma((heads, 7)), dma((heads, 7)),
        ],
        compiler_params=pltpu.CompilerParams(
            collective_id=0, has_side_effects=True, vmem_limit_bytes=60 * 2**20),
    )(
        dec_states,
        norm_gain.reshape(1, -1),
        query_weight.reshape(8, xcols, width),
        out_weight.reshape(heads, HD, 8 * xcols),
        enc_keys,
        enc_values,
    )


def solution(mesh):
    in_specs = (P("blk", "tp"), P(), P(None, "tp"), P("tp", None), P("blk", "tp"), P("blk", "tp"))
    return jax.shard_map(
        per_device, mesh=mesh, in_specs=in_specs, out_specs=P("blk", "tp"), check_vma=False
    )
```

```python
import math

import jax
import jax.numpy as jnp
from jax import lax
from jax.experimental import pallas as pl
from jax.experimental.pallas import tpu as pltpu
from jax.sharding import PartitionSpec as P

HD = 128
NORM_EPS = 1e-06
MESH = pl.DeviceIdType.MESH
NZ, NX = 8, 4
F32, BF16 = jnp.float32, jnp.bfloat16
LOG2E = 1.4426950408889634


def body(x_hbm, gain_ref, wq_hbm, wo_hbm, k_hbm, v_hbm, out_ref,
         kbuf, vbuf, vtmp, xbuf, wq, wobuf, qacc, ssacc, qbuf, acc, mbuf, lbuf,
         osend, ssend, orecv, srecv, att, oacc, wst,
         sbuf, lsem, zss, zrs, bss, brs, xss, xrs, wss, wrs, wbs, wbr, wys, wyr, qss, qrs,
         oss, ors, ass, ars):
    rows, xcols = x_hbm.shape
    toks = k_hbm.shape[0]
    heads = k_hbm.shape[1] // HD
    half = rows // 2
    blk, tp = lax.axis_index("blk"), lax.axis_index("tp")
    c = lax.rem(blk, 2)
    z = lax.rem(blk // 2, NZ)
    yl = blk // (2 * NZ)
    x, yh = tp // 2, lax.rem(tp, 2)

    def zdev(d):
        return ((yl * NZ + lax.rem(z + d + NZ, NZ)) * 2 + c, tp)

    def tpdev(dx, dy):
        return (blk, lax.rem(x + dx + NX, NX) * 2 + lax.rem(yh + dy, 2))

    def tpi(dx, dy):
        return lax.rem(x + dx + NX, NX) * 2 + lax.rem(yh + dy, 2)

    sib = (blk + 1 - 2 * c, tp)
    ypart = (blk + 2 * NZ - 4 * NZ * yl, tp)
    zsrc = lambda d: lax.rem(z + d + NZ, NZ)
    DX = (1, 3, 2)
    sends = []

    def rcopy(src, dst, ss, rs, dev):
        return pltpu.make_async_remote_copy(
            src_ref=src, dst_ref=dst, send_sem=ss, recv_sem=rs,
            device_id=dev, device_id_type=MESH)

    def send(src, dst, ss, rs, dev):
        cp = rcopy(src, dst, ss, rs, dev)
        cp.start()
        sends.append(cp)

    def await_recv(dst, ss, rs):
        rcopy(dst, dst, ss, rs, sib).wait_recv()

    def kslot(h, zz, cc):
        return kbuf.at[h, zz, pl.ds(cc * toks, toks), :]

    def vslot(h, zz, cc):
        return vbuf.at[h, zz, cc]

    kl = [pltpu.make_async_copy(k_hbm.at[:, pl.ds(h * HD, HD)], kslot(h, z, c), lsem.at[h]) for h in range(heads)]
    vl = [pltpu.make_async_copy(v_hbm.at[:, pl.ds(h * HD, HD)], vtmp.at[h], lsem.at[3 + h]) for h in range(heads)]
    xl = pltpu.make_async_copy(x_hbm, xbuf.at[tp], lsem.at[6])
    wql = pltpu.make_async_copy(wq_hbm, wq, lsem.at[7])
    wol = pltpu.make_async_copy(wo_hbm.at[:, :, pl.ds(pl.multiple_of(tp * xcols, HD), xcols)], wobuf.at[:, tp], lsem.at[8])
    kl[0].start()
    vl[0].start()
    xl.start()
    for h in range(1, heads):
        kl[h].start()
        vl[h].start()
    wql.start()
    wol.start()

    bar = pltpu.get_barrier_semaphore()
    peers = [zdev(1), zdev(-1), sib, ypart, tpdev(0, 1)] + [tpdev(dx, 0) for dx in DX]
    for dev in peers:
        pl.semaphore_signal(bar, inc=1, device_id=dev, device_id_type=MESH)
    pl.semaphore_wait(bar, len(peers))

    def zsend(h, s, d, kv):
        src_z = zsrc(-s if d == 0 else s)
        ref = kslot(h, src_z, c) if kv == 0 else vslot(h, src_z, c)
        send(ref, ref, zss.at[d, s, h, kv], zrs.at[d, s, h, kv], zdev(1 if d == 0 else -1))

    def bsend(h, src_z, slot, kv):
        ref = kslot(h, src_z, c) if kv == 0 else vslot(h, src_z, c)
        send(ref, ref, bss.at[slot, h, kv], brs.at[slot, h, kv], sib)

    def own(h):
        kl[h].wait()
        zsend(h, 0, 0, 0)
        vl[h].wait()
        vbuf[h, z, c] = vtmp[h].T
        zsend(h, 0, 1, 1)
        zsend(h, 0, 0, 1)
        zsend(h, 0, 1, 0)
        bsend(h, z, 0, 0)
        bsend(h, z, 0, 1)

    def slot_of(d, s):
        return 2 * s - 1 + d if s < 4 else 7

    ALL = ((0, 0), (1, 1), (0, 1), (1, 0))

    def arrive(h, s, order=ALL):
        for d, kv in order:
            if s == 4 and kv != d:
                continue
            src_z = zsrc(-s if d == 0 else s)
            ref = kslot(h, src_z, c) if kv == 0 else vslot(h, src_z, c)
            await_recv(ref, zss.at[d, s - 1, h, kv], zrs.at[d, s - 1, h, kv])
            if s < 3 or (s == 3 and kv == d):
                zsend(h, s, d, kv)
            bsend(h, src_z, slot_of(d, s), kv)

    def sib_arrive(h, s):
        if s == 0:
            lst = [(z, 0)]
        elif s == 4:
            lst = [(zsrc(4), 7)]
        else:
            lst = [(zsrc(-s), slot_of(0, s)), (zsrc(s), slot_of(1, s))]
        for src_z, slot in lst:
            await_recv(kslot(h, src_z, 1 - c), bss.at[slot, h, 0], brs.at[slot, h, 0])
            await_recv(vslot(h, src_z, 1 - c), bss.at[slot, h, 1], brs.at[slot, h, 1])

    XOWN_R, XOWN_L, XY, XP_R, XP_L, XOH_R, XOH_L, XPH_R, XPH_L = range(9)

    def xsend(ref, i, dx, dy):
        send(ref, ref, xss.at[i], xrs.at[i], tpdev(dx, dy))

    def xwait(ref, i):
        await_recv(ref, xss.at[i], xrs.at[i])

    def xfull(t):
        return xbuf.at[t]

    def xtop(t):
        return xbuf.at[t, pl.ds(0, half), :]

    def xbot(t):
        return xbuf.at[t, pl.ds(half, half), :]

    def qblock(t, first=False):
        xf = xbuf[t].astype(F32)
        sq = xf * xf
        part = sq[:, 0:HD]
        for j in range(1, xcols // HD):
            part = part + sq[:, j * HD:(j + 1) * HD]
        g = gain_ref[:, pl.ds(pl.multiple_of(t * xcols, HD), xcols)]
        xg = (xf * g).astype(BF16)
        prod = jnp.dot(xg, wq[t], preferred_element_type=F32)
        if first:
            ssacc[...] = part
            qacc[...] = prod
        else:
            ssacc[...] += part
            qacc[...] += prod

    def init_state():
        mbuf[...] = jnp.full(mbuf.shape, -1e30, F32)
        lbuf[...] = jnp.zeros(lbuf.shape, F32)
        acc[...] = jnp.zeros(acc.shape, F32)

    def update(h, r, s, vv):
        mo = mbuf[h, r]
        mn = jnp.maximum(mo, jnp.max(s, axis=0, keepdims=True))
        p = jnp.exp2(s - mn).astype(BF16)
        f = jnp.exp2(mo - mn)
        ones = jnp.ones((16, vv.shape[1]), BF16)
        o = jnp.dot(jnp.concatenate([vv, ones], axis=0), p, preferred_element_type=F32)
        lbuf[h, r] = lbuf[h, r] * f + o[HD:HD + 1]
        acc[h, r] = acc[h, r] * f + o[:HD]
        mbuf[h, r] = mn

    cur = []

    def stream(items):
        par = (cur[0][1] + 1) % 2 if cur else 0
        old, old_par = cur.pop() if cur else ((), 0)
        for i in range(2):
            if items:
                h, d, r = items[i]
                sbuf[2 * par + i] = scores(h, zsrc(d), r)
            if old:
                h, d, r = old[i]
                update(h, r, sbuf[2 * old_par + i], values(h, zsrc(d)))
        if items:
            cur.append((items, par))

    def feed(h, d):
        stream(((h, d, 1), (h, d, 0)))

    def feed_rows(h, r, d0, d1):
        stream(((h, d0, r), (h, d1, r)))

    def flush_last():
        old, par = cur.pop()
        for i in range(2):
            h, d, r = old[i]
            update(h, r, sbuf[2 * par + i], values(h, zsrc(d)))
            if i == 0:
                finish_partner(h)

    def scores(h, zz, r):
        return lax.dot_general(kbuf[h, zz], qbuf[h, r], (((1,), (1,)), ((), ())), preferred_element_type=F32)

    def values(h, zz):
        return jnp.concatenate([vbuf[h, zz, 0], vbuf[h, zz, 1]], axis=1)

    def finish_partner(h):
        osend[h] = acc[h, 1].astype(BF16)
        ssend[h, 0:1] = mbuf[h, 1]
        ssend[h, 1:2] = lbuf[h, 1]
        send(osend.at[h], orecv.at[h], oss.at[h, 0], ors.at[h, 0], ypart)
        send(ssend.at[h], srecv.at[h], oss.at[h, 1], ors.at[h, 1], ypart)

    def merge(h):
        await_recv(orecv.at[h], oss.at[h, 0], ors.at[h, 0])
        await_recv(srecv.at[h], oss.at[h, 1], ors.at[h, 1])
        ma, mb = mbuf[h, 0], srecv[h, 0:1]
        m = jnp.maximum(ma, mb)
        fa, fb = jnp.exp2(ma - m), jnp.exp2(mb - m)
        tot = lbuf[h, 0] * fa + srecv[h, 1:2] * fb
        o = (acc[h, 0] * fa + orecv[h].astype(F32) * fb) / tot
        att[h, tp] = o.T.astype(BF16)
        att_one(h, tp, 3, 0, 1)
        att_send(h, tp, 0)

    def att_one(h, t, i, dx, dy):
        send(att.at[h, t], att.at[h, t], ass.at[h, i], ars.at[h, i], tpdev(dx, dy))

    def att_send(h, t, base):
        for i in (2, 0, 1):
            att_one(h, t, base + i, DX[i], 0)

    def att_wait(h, i, dx, dy):
        await_recv(att.at[h, tpi(-dx, dy)], ass.at[h, i], ars.at[h, i])

    def att_relay(h):
        att_wait(h, 3, 0, 1)
        att_send(h, tpi(0, 1), 4)

    def out_part(h, first=False):
        for i, dx in enumerate(DX):
            att_wait(h, i, dx, 0)
        for i, dx in enumerate(DX):
            att_wait(h, 4 + i, dx, 1)
        a = jnp.concatenate([att[h, t] for t in range(8)], axis=1)
        w = wobuf[h].reshape(8 * HD, xcols)
        prod = jnp.dot(a, w, preferred_element_type=F32)
        if first:
            oacc[...] = prod
        else:
            oacc[...] += prod

    hh = HD // 4

    def wslot(t, cc, yy):
        return wobuf.at[:, t, pl.ds((2 * cc + yy) * hh, hh), :]

    def wsrc(t):
        return wo_hbm.at[:, pl.ds((2 * c + yl) * hh, hh), pl.ds(pl.multiple_of(t * xcols, HD), xcols)]

    def w_own(i):
        send(wsrc(tpi(DX[i], 0)), wslot(tp, c, yl), wss.at[i], wrs.at[i], tpdev(DX[i], 0))

    def w_y():
        for i, dx in enumerate(DX):
            send(wsrc(tpi(dx, 1)), wst.at[i], wss.at[7 + i], wrs.at[7 + i], tpdev(0, 1))
        send(wsrc(tpi(0, 1)), wslot(tp, c, yl), wss.at[6], wrs.at[6], tpdev(0, 1))

    def w_relay(i):
        await_recv(wst.at[i], wss.at[7 + i], wrs.at[7 + i])
        send(wst.at[i], wslot(tpi(0, 1), c, yl), wss.at[3 + i], wrs.at[3 + i], tpdev(DX[i], 0))

    def w_from(i):
        return tpi(0, 1) if i == 6 else tpi(-DX[i % 3], i // 3)

    def wfwd(i):
        ref = wslot(w_from(i), c, yl)
        await_recv(ref, wss.at[i], wrs.at[i])
        send(ref, ref, wys.at[i], wyr.at[i], ypart)
        send(ref, ref, wbs.at[0, i], wbr.at[0, i], sib)

    def wfwd2():
        for i in W_ORDER:
            ref = wslot(w_from(i), c, 1 - yl)
            await_recv(ref, wys.at[i], wyr.at[i])
            send(ref, ref, wbs.at[1, i], wbr.at[1, i], sib)

    def wdone():
        wol.wait()
        for j in range(2):
            for i in W_ORDER:
                ref = wslot(w_from(i), 1 - c, yl if j == 0 else 1 - yl)
                await_recv(ref, wbs.at[j, i], wbr.at[j, i])

    W_ORDER = (0, 1, 6, 2, 3, 4, 5)
    tl, tr, t2 = tpi(-1, 0), tpi(1, 0), tpi(2, 0)
    pt, ptl, ptr, pt2 = tpi(0, 1), tpi(-1, 1), tpi(1, 1), tpi(2, 1)

    own(0)
    xl.wait()
    xsend(xfull(tp), XOWN_R, 1, 0)
    xsend(xfull(tp), XOWN_L, -1, 0)
    xsend(xfull(tp), XY, 0, 1)
    own(1)
    w_y()
    w_own(0)
    w_own(1)
    init_state()
    wql.wait()
    qblock(tp, True)
    arrive(0, 1)
    own(2)
    xwait(xfull(tl), XOWN_R)
    xsend(xtop(tl), XOH_R, 1, 0)
    xwait(xfull(tr), XOWN_L)
    xsend(xbot(tr), XOH_L, -1, 0)
    xwait(xfull(pt), XY)
    xsend(xfull(pt), XP_R, 1, 0)
    xsend(xfull(pt), XP_L, -1, 0)
    qblock(tl)
    qblock(tr)
    qblock(pt)
    arrive(0, 2)
    arrive(1, 1)
    xwait(xtop(t2), XOH_R)
    xwait(xbot(t2), XOH_L)
    qblock(t2)
    wfwd(0)
    wfwd(1)
    xwait(xfull(ptl), XP_R)
    xsend(xtop(ptl), XPH_R, 1, 0)
    xwait(xfull(ptr), XP_L)
    xsend(xbot(ptr), XPH_L, -1, 0)
    w_own(2)
    qblock(ptl)
    qblock(ptr)
    arrive(0, 3)
    w_relay(0)
    w_relay(1)
    w_relay(2)
    wfwd(6)
    arrive(1, 2)
    arrive(2, 1)
    xwait(xtop(pt2), XPH_R)
    xwait(xbot(pt2), XPH_L)
    qblock(pt2)

    mean_sq = jnp.sum(ssacc[...], axis=1, keepdims=True) * (1.0 / (8 * xcols))
    scale = lax.rsqrt(mean_sq + NORM_EPS) * (LOG2E / math.sqrt(HD))
    for h in range(heads):
        qbuf[h, 0] = (qacc[:, h * HD:(h + 1) * HD] * scale).astype(BF16)
        send(qbuf.at[h, 0], qbuf.at[h, 1], qss.at[h], qrs.at[h], ypart)

    def qwait(h):
        await_recv(qbuf.at[h, 1], qss.at[h], qrs.at[h])

    sib_arrive(0, 0)
    sib_arrive(0, 1)
    sib_arrive(0, 2)
    feed_rows(0, 0, 0, -1)
    arrive(0, 4)
    feed_rows(0, 0, 1, -2)
    wfwd(2)
    sib_arrive(0, 3)
    feed_rows(0, 0, 2, -3)
    sib_arrive(1, 0)
    sib_arrive(1, 1)
    feed_rows(1, 0, 0, -1)
    sib_arrive(0, 4)
    feed_rows(0, 0, 3, 4)
    qwait(0)
    feed_rows(0, 1, 0, -1)
    feed_rows(0, 1, 1, -2)
    arrive(1, 3)
    feed_rows(0, 1, 2, -3)
    feed_rows(0, 1, 3, 4)
    qwait(1)
    feed_rows(1, 1, 0, -1)
    finish_partner(0)
    wfwd(3)
    feed(1, 1)
    sib_arrive(1, 2)
    feed(1, -2)
    feed(1, 2)
    arrive(2, 2)
    wfwd(4)
    sib_arrive(1, 3)
    feed(1, -3)
    feed(1, 3)
    merge(0)
    qwait(2)
    sib_arrive(2, 0)
    sib_arrive(2, 1)
    feed(2, 0)
    arrive(1, 4)
    feed(2, -1)
    feed(2, 1)
    arrive(2, 3, ALL[:2])
    sib_arrive(1, 4)
    feed(1, 4)
    sib_arrive(2, 2)
    feed(2, -2)
    finish_partner(1)
    feed(2, 2)
    wfwd(5)
    arrive(2, 3, ALL[2:])
    att_relay(0)
    sib_arrive(2, 3)
    feed(2, -3)
    feed(2, 3)
    arrive(2, 4)
    merge(1)
    sib_arrive(2, 4)
    feed(2, 4)
    flush_last()
    att_relay(1)
    merge(2)
    wfwd2()
    att_relay(2)
    wdone()
    out_part(0, True)
    out_part(1)
    out_part(2)
    out_ref[...] = oacc[...].astype(BF16)
    for cp in sends:
        cp.wait_send()


def per_device(dec_states, norm_gain, query_weight, out_weight, enc_keys, enc_values):
    rows, xcols = dec_states.shape
    toks, width = enc_keys.shape
    heads = width // HD
    vm = pltpu.VMEM
    dma = pltpu.SemaphoreType.DMA
    hbm = pl.BlockSpec(memory_space=pltpu.HBM)
    inv = pl.BlockSpec(memory_space=pltpu.VMEM)
    return pl.pallas_call(
        body,
        out_shape=pltpu.VMEM((rows, xcols), BF16),
        in_specs=[hbm, inv, hbm, hbm, hbm, hbm],
        out_specs=inv,
        scratch_shapes=[
            vm((heads, NZ, 2 * toks, HD), BF16),
            vm((heads, NZ, 2, HD, toks), BF16),
            vm((heads, toks, HD), BF16),
            vm((8, rows, xcols), BF16),
            vm((8, xcols, width), BF16),
            vm((heads, 8, HD, xcols), BF16),
            vm((rows, width), F32),
            vm((rows, HD), F32),
            vm((heads, 2, rows, HD), BF16),
            vm((heads, 2, HD, rows), F32),
            vm((heads, 2, 1, rows), F32),
            vm((heads, 2, 1, rows), F32),
            vm((heads, HD, rows), BF16),
            vm((heads, 8, rows), F32),
            vm((heads, HD, rows), BF16),
            vm((heads, 8, rows), F32),
            vm((heads, 8, rows, HD), BF16),
            vm((rows, xcols), F32),
            vm((3, heads, HD // 4, xcols), BF16),
            vm((4, 2 * toks, rows), F32),
            dma((9,)),
            dma((2, 4, heads, 2)), dma((2, 4, heads, 2)),
            dma((8, heads, 2)), dma((8, heads, 2)),
            dma((9,)), dma((9,)),
            dma((10,)), dma((10,)),
            dma((2, 7)), dma((2, 7)),
            dma((7,)), dma((7,)),
            dma((heads,)), dma((heads,)),
            dma((heads, 2)), dma((heads, 2)),
            dma((heads, 7)), dma((heads, 7)),
        ],
        compiler_params=pltpu.CompilerParams(
            collective_id=0, has_side_effects=True, vmem_limit_bytes=60 * 2**20),
    )(
        dec_states,
        norm_gain.reshape(1, -1),
        query_weight.reshape(8, xcols, width),
        out_weight.reshape(heads, HD, 8 * xcols),
        enc_keys,
        enc_values,
    )


def solution(mesh):
    in_specs = (P("blk", "tp"), P(), P(None, "tp"), P("tp", None), P("blk", "tp"), P("blk", "tp"))
    return jax.shard_map(
        per_device, mesh=mesh, in_specs=in_specs, out_specs=P("blk", "tp"), check_vma=False
    )
```

```python
import math

import jax
import jax.numpy as jnp
from jax import lax
from jax.experimental import pallas as pl
from jax.experimental.pallas import tpu as pltpu
from jax.sharding import PartitionSpec as P

HD = 128
NORM_EPS = 1e-06
MESH = pl.DeviceIdType.MESH
NZ, NX = 8, 4
F32, BF16 = jnp.float32, jnp.bfloat16
LOG2E = 1.4426950408889634


def body(x_hbm, gain_ref, wq_hbm, wo_hbm, k_hbm, v_hbm, out_ref,
         kbuf, vbuf, vtmp, xbuf, wq, wobuf, qacc, ssacc, qbuf, acc, mbuf, lbuf,
         osend, ssend, psend, tsend, orecv, srecv, att, oacc, wst,
         sbuf, lsem, zss, zrs, bss, brs, xss, xrs, wss, wrs, wbs, wbr, wys, wyr, qss, qrs,
         oss, ors, ass, ars):
    rows, xcols = x_hbm.shape
    toks = k_hbm.shape[0]
    heads = k_hbm.shape[1] // HD
    half = rows // 2
    blk, tp = lax.axis_index("blk"), lax.axis_index("tp")
    c = lax.rem(blk, 2)
    z = lax.rem(blk // 2, NZ)
    yl = blk // (2 * NZ)
    x, yh = tp // 2, lax.rem(tp, 2)

    def zdev(d):
        return ((yl * NZ + lax.rem(z + d + NZ, NZ)) * 2 + c, tp)

    def tpdev(dx, dy):
        return (blk, lax.rem(x + dx + NX, NX) * 2 + lax.rem(yh + dy, 2))

    def tpi(dx, dy):
        return lax.rem(x + dx + NX, NX) * 2 + lax.rem(yh + dy, 2)

    sib = (blk + 1 - 2 * c, tp)
    ypart = (blk + 2 * NZ - 4 * NZ * yl, tp)
    ydiag = (blk + 2 * NZ - 4 * NZ * yl, tp + 1 - 2 * yh)
    zsrc = lambda d: lax.rem(z + d + NZ, NZ)
    DX = (1, 3, 2)
    sends = []

    def rcopy(src, dst, ss, rs, dev):
        return pltpu.make_async_remote_copy(
            src_ref=src, dst_ref=dst, send_sem=ss, recv_sem=rs,
            device_id=dev, device_id_type=MESH)

    def send(src, dst, ss, rs, dev):
        cp = rcopy(src, dst, ss, rs, dev)
        cp.start()
        sends.append(cp)

    def await_recv(dst, ss, rs):
        rcopy(dst, dst, ss, rs, sib).wait_recv()

    def kslot(h, zz, cc):
        return kbuf.at[h, zz, pl.ds(cc * toks, toks), :]

    def vslot(h, zz, cc):
        return vbuf.at[h, zz, cc]

    kl = [pltpu.make_async_copy(k_hbm.at[:, pl.ds(h * HD, HD)], kslot(h, z, c), lsem.at[h]) for h in range(heads)]
    vl = [pltpu.make_async_copy(v_hbm.at[:, pl.ds(h * HD, HD)], vtmp.at[h], lsem.at[3 + h]) for h in range(heads)]
    xl = pltpu.make_async_copy(x_hbm, xbuf.at[tp], lsem.at[6])
    wql = pltpu.make_async_copy(wq_hbm, wq, lsem.at[7])
    wol = pltpu.make_async_copy(wo_hbm.at[:, :, pl.ds(pl.multiple_of(tp * xcols, HD), xcols)], wobuf.at[:, tp], lsem.at[8])
    kl[0].start()
    vl[0].start()
    xl.start()
    for h in range(1, heads):
        kl[h].start()
        vl[h].start()
    wql.start()
    wol.start()

    bar = pltpu.get_barrier_semaphore()
    peers = [zdev(1), zdev(-1), sib, ypart, ydiag, tpdev(0, 1)] + [tpdev(dx, 0) for dx in DX]
    for dev in peers:
        pl.semaphore_signal(bar, inc=1, device_id=dev, device_id_type=MESH)
    pl.semaphore_wait(bar, len(peers))

    def zsend(h, s, d, kv):
        src_z = zsrc(-s if d == 0 else s)
        ref = kslot(h, src_z, c) if kv == 0 else vslot(h, src_z, c)
        send(ref, ref, zss.at[d, s, h, kv], zrs.at[d, s, h, kv], zdev(1 if d == 0 else -1))

    def bsend(h, src_z, slot, kv):
        ref = kslot(h, src_z, c) if kv == 0 else vslot(h, src_z, c)
        send(ref, ref, bss.at[slot, h, kv], brs.at[slot, h, kv], sib)

    def own(h):
        kl[h].wait()
        zsend(h, 0, 0, 0)
        vl[h].wait()
        vbuf[h, z, c] = vtmp[h].T
        zsend(h, 0, 1, 1)
        zsend(h, 0, 0, 1)
        zsend(h, 0, 1, 0)
        bsend(h, z, 0, 0)
        bsend(h, z, 0, 1)

    def slot_of(d, s):
        return 2 * s - 1 + d if s < 4 else 7

    ALL = ((0, 0), (1, 1), (0, 1), (1, 0))

    def arrive(h, s, order=ALL):
        for d, kv in order:
            if s == 4 and kv != d:
                continue
            src_z = zsrc(-s if d == 0 else s)
            ref = kslot(h, src_z, c) if kv == 0 else vslot(h, src_z, c)
            await_recv(ref, zss.at[d, s - 1, h, kv], zrs.at[d, s - 1, h, kv])
            if s < 3 or (s == 3 and kv == d):
                zsend(h, s, d, kv)
            bsend(h, src_z, slot_of(d, s), kv)

    def sib_arrive(h, s):
        if s == 0:
            lst = [(z, 0)]
        elif s == 4:
            lst = [(zsrc(4), 7)]
        else:
            lst = [(zsrc(-s), slot_of(0, s)), (zsrc(s), slot_of(1, s))]
        for src_z, slot in lst:
            await_recv(kslot(h, src_z, 1 - c), bss.at[slot, h, 0], brs.at[slot, h, 0])
            await_recv(vslot(h, src_z, 1 - c), bss.at[slot, h, 1], brs.at[slot, h, 1])

    XOWN_R, XOWN_L, XY, XP_R, XP_L, XOH_R, XOH_L, XPH_R, XPH_L = range(9)

    def xsend(ref, i, dx, dy):
        send(ref, ref, xss.at[i], xrs.at[i], tpdev(dx, dy))

    def xwait(ref, i):
        await_recv(ref, xss.at[i], xrs.at[i])

    def xfull(t):
        return xbuf.at[t]

    def xtop(t):
        return xbuf.at[t, pl.ds(0, half), :]

    def xbot(t):
        return xbuf.at[t, pl.ds(half, half), :]

    def qblock(t, first=False):
        xf = xbuf[t].astype(F32)
        sq = xf * xf
        part = sq[:, 0:HD]
        for j in range(1, xcols // HD):
            part = part + sq[:, j * HD:(j + 1) * HD]
        g = gain_ref[:, pl.ds(pl.multiple_of(t * xcols, HD), xcols)]
        xg = (xf * g).astype(BF16)
        prod = jnp.dot(xg, wq[t], preferred_element_type=F32)
        if first:
            ssacc[...] = part
            qacc[...] = prod
        else:
            ssacc[...] += part
            qacc[...] += prod

    def init_state():
        mbuf[...] = jnp.full(mbuf.shape, -1e30, F32)
        lbuf[...] = jnp.zeros(lbuf.shape, F32)
        acc[...] = jnp.zeros(acc.shape, F32)

    def update(h, r, s, vv):
        mo = mbuf[h, r]
        mn = jnp.maximum(mo, jnp.max(s, axis=0, keepdims=True))
        p = jnp.exp2(s - mn).astype(BF16)
        f = jnp.exp2(mo - mn)
        ones = jnp.ones((16, vv.shape[1]), BF16)
        o = jnp.dot(jnp.concatenate([vv, ones], axis=0), p, preferred_element_type=F32)
        lbuf[h, r] = lbuf[h, r] * f + o[HD:HD + 1]
        acc[h, r] = acc[h, r] * f + o[:HD]
        mbuf[h, r] = mn

    cur = []

    def stream(items):
        par = (cur[0][1] + 1) % 2 if cur else 0
        old, old_par = cur.pop() if cur else ((), 0)
        for i in range(2):
            if items:
                h, d, r = items[i]
                sbuf[2 * par + i] = scores(h, zsrc(d), r)
            if old:
                h, d, r = old[i]
                update(h, r, sbuf[2 * old_par + i], values(h, zsrc(d)))
        if items:
            cur.append((items, par))

    def feed(h, d):
        stream(((h, d, 1), (h, d, 0)))

    def feed_rows(h, r, d0, d1):
        stream(((h, d0, r), (h, d1, r)))

    def flush_last():
        old, par = cur.pop()
        for i in range(2):
            h, d, r = old[i]
            update(h, r, sbuf[2 * par + i], values(h, zsrc(d)))
            if i == 0:
                finish_partner(h)
        finish_own(h)

    def scores(h, zz, r):
        return lax.dot_general(kbuf[h, zz], qbuf[h, r], (((1,), (1,)), ((), ())), preferred_element_type=F32)

    def values(h, zz):
        return jnp.concatenate([vbuf[h, zz, 0], vbuf[h, zz, 1]], axis=1)

    def finish_partner(h):
        osend[h] = acc[h, 1].astype(BF16)
        ssend[h, 0:1] = mbuf[h, 1]
        ssend[h, 1:2] = lbuf[h, 1]
        send(ssend.at[h], srecv.at[h, 0], oss.at[h, 0], ors.at[h, 0], ypart)
        send(osend.at[h], orecv.at[h, 0], oss.at[h, 1], ors.at[h, 1], ypart)
        send(ssend.at[h], srecv.at[h, 1], oss.at[h, 2], ors.at[h, 2], ydiag)
        send(osend.at[h], orecv.at[h, 1], oss.at[h, 3], ors.at[h, 3], ydiag)

    def finish_own(h):
        psend[h] = acc[h, 0].astype(BF16)
        tsend[h, 0:1] = mbuf[h, 0]
        tsend[h, 1:2] = lbuf[h, 0]
        send(tsend.at[h], srecv.at[h, 2], oss.at[h, 4], ors.at[h, 4], tpdev(0, 1))
        send(psend.at[h], orecv.at[h, 2], oss.at[h, 5], ors.at[h, 5], tpdev(0, 1))

    def owait(h, j):
        await_recv(srecv.at[h, j], oss.at[h, 2 * j], ors.at[h, 2 * j])
        await_recv(orecv.at[h, j], oss.at[h, 2 * j + 1], ors.at[h, 2 * j + 1])

    def combine(h, t, ma, la, oa, mb, lb, ob):
        m = jnp.maximum(ma, mb)
        fa, fb = jnp.exp2(ma - m), jnp.exp2(mb - m)
        tot = la * fa + lb * fb
        att[h, t] = ((oa * fa + ob * fb) / tot).T.astype(BF16)

    def merge(h):
        owait(h, 0)
        combine(h, tp, mbuf[h, 0], lbuf[h, 0], acc[h, 0],
                srecv[h, 0, 0:1], srecv[h, 0, 1:2], orecv[h, 0].astype(F32))
        att_send(h, tp, 0)

    def att_relay(h):
        owait(h, 1)
        owait(h, 2)
        t = tpi(0, 1)
        combine(h, t, srecv[h, 2, 0:1], srecv[h, 2, 1:2], orecv[h, 2].astype(F32),
                srecv[h, 1, 0:1], srecv[h, 1, 1:2], orecv[h, 1].astype(F32))
        att_send(h, t, 4)

    def att_one(h, t, i, dx, dy):
        send(att.at[h, t], att.at[h, t], ass.at[h, i], ars.at[h, i], tpdev(dx, dy))

    def att_send(h, t, base):
        for i in (2, 0, 1):
            att_one(h, t, base + i, DX[i], 0)

    def att_wait(h, i, dx, dy):
        await_recv(att.at[h, tpi(-dx, dy)], ass.at[h, i], ars.at[h, i])

    def out_part(h, first=False):
        for i, dx in enumerate(DX):
            att_wait(h, i, dx, 0)
        for i, dx in enumerate(DX):
            att_wait(h, 4 + i, dx, 1)
        a = jnp.concatenate([att[h, t] for t in range(8)], axis=1)
        w = wobuf[h].reshape(8 * HD, xcols)
        prod = jnp.dot(a, w, preferred_element_type=F32)
        if first:
            oacc[...] = prod
        else:
            oacc[...] += prod

    hh = HD // 4

    def wslot(t, cc, yy):
        return wobuf.at[:, t, pl.ds((2 * cc + yy) * hh, hh), :]

    def wsrc(t):
        return wo_hbm.at[:, pl.ds((2 * c + yl) * hh, hh), pl.ds(pl.multiple_of(t * xcols, HD), xcols)]

    def w_own(i):
        send(wsrc(tpi(DX[i], 0)), wslot(tp, c, yl), wss.at[i], wrs.at[i], tpdev(DX[i], 0))

    def w_y():
        for i, dx in enumerate(DX):
            send(wsrc(tpi(dx, 1)), wst.at[i], wss.at[7 + i], wrs.at[7 + i], tpdev(0, 1))
        send(wsrc(tpi(0, 1)), wslot(tp, c, yl), wss.at[6], wrs.at[6], tpdev(0, 1))

    def w_relay(i):
        await_recv(wst.at[i], wss.at[7 + i], wrs.at[7 + i])
        send(wst.at[i], wslot(tpi(0, 1), c, yl), wss.at[3 + i], wrs.at[3 + i], tpdev(DX[i], 0))

    def w_from(i):
        return tpi(0, 1) if i == 6 else tpi(-DX[i % 3], i // 3)

    def wfwd(i):
        ref = wslot(w_from(i), c, yl)
        await_recv(ref, wss.at[i], wrs.at[i])
        send(ref, ref, wys.at[i], wyr.at[i], ypart)
        send(ref, ref, wbs.at[0, i], wbr.at[0, i], sib)

    def wfwd2():
        for i in W_ORDER:
            ref = wslot(w_from(i), c, 1 - yl)
            await_recv(ref, wys.at[i], wyr.at[i])
            send(ref, ref, wbs.at[1, i], wbr.at[1, i], sib)

    def wdone():
        wol.wait()
        for j in range(2):
            for i in W_ORDER:
                ref = wslot(w_from(i), 1 - c, yl if j == 0 else 1 - yl)
                await_recv(ref, wbs.at[j, i], wbr.at[j, i])

    W_ORDER = (0, 1, 6, 2, 3, 4, 5)
    tl, tr, t2 = tpi(-1, 0), tpi(1, 0), tpi(2, 0)
    pt, ptl, ptr, pt2 = tpi(0, 1), tpi(-1, 1), tpi(1, 1), tpi(2, 1)

    own(0)
    xl.wait()
    xsend(xfull(tp), XOWN_R, 1, 0)
    xsend(xfull(tp), XOWN_L, -1, 0)
    xsend(xfull(tp), XY, 0, 1)
    own(1)
    w_y()
    w_own(0)
    w_own(1)
    init_state()
    wql.wait()
    qblock(tp, True)
    arrive(0, 1)
    own(2)
    xwait(xfull(tl), XOWN_R)
    xsend(xtop(tl), XOH_R, 1, 0)
    xwait(xfull(tr), XOWN_L)
    xsend(xbot(tr), XOH_L, -1, 0)
    xwait(xfull(pt), XY)
    xsend(xfull(pt), XP_R, 1, 0)
    xsend(xfull(pt), XP_L, -1, 0)
    qblock(tl)
    qblock(tr)
    qblock(pt)
    arrive(0, 2)
    arrive(1, 1)
    xwait(xtop(t2), XOH_R)
    xwait(xbot(t2), XOH_L)
    qblock(t2)
    wfwd(0)
    wfwd(1)
    xwait(xfull(ptl), XP_R)
    xsend(xtop(ptl), XPH_R, 1, 0)
    xwait(xfull(ptr), XP_L)
    xsend(xbot(ptr), XPH_L, -1, 0)
    w_own(2)
    qblock(ptl)
    qblock(ptr)
    arrive(0, 3)
    w_relay(0)
    w_relay(1)
    w_relay(2)
    wfwd(6)
    arrive(1, 2)
    arrive(2, 1)
    xwait(xtop(pt2), XPH_R)
    xwait(xbot(pt2), XPH_L)
    qblock(pt2)

    mean_sq = jnp.sum(ssacc[...], axis=1, keepdims=True) * (1.0 / (8 * xcols))
    scale = lax.rsqrt(mean_sq + NORM_EPS) * (LOG2E / math.sqrt(HD))
    for h in range(heads):
        qbuf[h, 0] = (qacc[:, h * HD:(h + 1) * HD] * scale).astype(BF16)
        send(qbuf.at[h, 0], qbuf.at[h, 1], qss.at[h], qrs.at[h], ypart)

    def qwait(h):
        await_recv(qbuf.at[h, 1], qss.at[h], qrs.at[h])

    sib_arrive(0, 0)
    sib_arrive(0, 1)
    sib_arrive(0, 2)
    feed_rows(0, 0, 0, -1)
    arrive(0, 4)
    feed_rows(0, 0, 1, -2)
    wfwd(2)
    sib_arrive(0, 3)
    feed_rows(0, 0, 2, -3)
    sib_arrive(1, 0)
    sib_arrive(1, 1)
    feed_rows(1, 0, 0, -1)
    sib_arrive(0, 4)
    feed_rows(0, 0, 3, 4)
    qwait(0)
    feed_rows(0, 1, 0, -1)
    feed_rows(0, 1, 1, -2)
    arrive(1, 3)
    feed_rows(0, 1, 2, -3)
    feed_rows(0, 1, 3, 4)
    qwait(1)
    feed_rows(1, 1, 0, -1)
    finish_partner(0)
    finish_own(0)
    wfwd(3)
    feed(1, 1)
    sib_arrive(1, 2)
    feed(1, -2)
    feed(1, 2)
    arrive(2, 2)
    wfwd(4)
    sib_arrive(1, 3)
    feed(1, -3)
    feed(1, 3)
    merge(0)
    qwait(2)
    sib_arrive(2, 0)
    sib_arrive(2, 1)
    feed(2, 0)
    arrive(1, 4)
    feed(2, -1)
    feed(2, 1)
    arrive(2, 3, ALL[:2])
    sib_arrive(1, 4)
    feed(1, 4)
    sib_arrive(2, 2)
    feed(2, -2)
    finish_partner(1)
    finish_own(1)
    feed(2, 2)
    wfwd(5)
    arrive(2, 3, ALL[2:])
    att_relay(0)
    sib_arrive(2, 3)
    feed(2, -3)
    feed(2, 3)
    arrive(2, 4)
    merge(1)
    sib_arrive(2, 4)
    feed(2, 4)
    flush_last()
    att_relay(1)
    merge(2)
    wfwd2()
    att_relay(2)
    wdone()
    out_part(0, True)
    out_part(1)
    out_part(2)
    out_ref[...] = oacc[...].astype(BF16)
    for cp in sends:
        cp.wait_send()


def per_device(dec_states, norm_gain, query_weight, out_weight, enc_keys, enc_values):
    rows, xcols = dec_states.shape
    toks, width = enc_keys.shape
    heads = width // HD
    vm = pltpu.VMEM
    dma = pltpu.SemaphoreType.DMA
    hbm = pl.BlockSpec(memory_space=pltpu.HBM)
    inv = pl.BlockSpec(memory_space=pltpu.VMEM)
    return pl.pallas_call(
        body,
        out_shape=pltpu.VMEM((rows, xcols), BF16),
        in_specs=[hbm, inv, hbm, hbm, hbm, hbm],
        out_specs=inv,
        scratch_shapes=[
            vm((heads, NZ, 2 * toks, HD), BF16),
            vm((heads, NZ, 2, HD, toks), BF16),
            vm((heads, toks, HD), BF16),
            vm((8, rows, xcols), BF16),
            vm((8, xcols, width), BF16),
            vm((heads, 8, HD, xcols), BF16),
            vm((rows, width), F32),
            vm((rows, HD), F32),
            vm((heads, 2, rows, HD), BF16),
            vm((heads, 2, HD, rows), F32),
            vm((heads, 2, 1, rows), F32),
            vm((heads, 2, 1, rows), F32),
            vm((heads, HD, rows), BF16),
            vm((heads, 8, rows), F32),
            vm((heads, HD, rows), BF16),
            vm((heads, 8, rows), F32),
            vm((heads, 3, HD, rows), BF16),
            vm((heads, 3, 8, rows), F32),
            vm((heads, 8, rows, HD), BF16),
            vm((rows, xcols), F32),
            vm((3, heads, HD // 4, xcols), BF16),
            vm((4, 2 * toks, rows), F32),
            dma((9,)),
            dma((2, 4, heads, 2)), dma((2, 4, heads, 2)),
            dma((8, heads, 2)), dma((8, heads, 2)),
            dma((9,)), dma((9,)),
            dma((10,)), dma((10,)),
            dma((2, 7)), dma((2, 7)),
            dma((7,)), dma((7,)),
            dma((heads,)), dma((heads,)),
            dma((heads, 6)), dma((heads, 6)),
            dma((heads, 7)), dma((heads, 7)),
        ],
        compiler_params=pltpu.CompilerParams(
            collective_id=0, has_side_effects=True, vmem_limit_bytes=60 * 2**20),
    )(
        dec_states,
        norm_gain.reshape(1, -1),
        query_weight.reshape(8, xcols, width),
        out_weight.reshape(heads, HD, 8 * xcols),
        enc_keys,
        enc_values,
    )


def solution(mesh):
    in_specs = (P("blk", "tp"), P(), P(None, "tp"), P("tp", None), P("blk", "tp"), P("blk", "tp"))
    return jax.shard_map(
        per_device, mesh=mesh, in_specs=in_specs, out_specs=P("blk", "tp"), check_vma=False
    )
```
